32 devices in a mesh: seq: 4 (over y, core), lat: 4 (over z), batch: 2 (over x).
Axes of the slice: x: 2, y: 2, z: 4, core: 2. Of those that a mesh axis runs over, the one named last changes fastest.
Arguments:
- activations: bfloat16 [2, 1024, 3584], P('batch', 'seq'), may hold values from -6 to 6
- dictionary: bfloat16 [4096, 3584], P('lat'), may hold values from -0.09375 to 0.09375
- topk_ids: int32 [2, 1024, 64], P('batch', 'seq'), may hold values from 0 to 4095, as said below
- kernel_taps: float32 [9, 4096], P(None, 'lat'), may hold values from -2 to 2
- enc_bias: float32 [4096], P('lat'), may hold values from -3 to 3
Outputs:
- grad_dictionary: float32 [4096, 3584], P('lat', ('seq', 'batch'))
- grad_taps: float32 [9, 4096], P(None, 'lat')
- grad_bias: float32 [4096], P('lat')
The draws below stay inside these ranges and needn't reach their ends.
Inputs may be any that keep to these rules, and one draw needn't show every extreme that they name: `topk_ids`: each position names 64 different latents.
All inputs are finite; a program needn't handle non-finite values.
Results may differ from the reference program's by a relative error of at most 0.017.
Values may be sent and summed in bfloat16 or wider, within the bound.
No kernel may reach another device: no remote copies, remote signals or barrier semaphores. Data moves between devices by JAX's collectives and lax.ppermute only.
A program may use at most 128 MiB of HBM per device.

```python
import jax
import jax.numpy as jnp
from jax import lax

D = 3584
LAT_DEV = 1024
TOPK = 64
TAPS = 9
HALF = 4
LATENTS = 4096
LENGTH = 1024
SEQS = 2
N_SEQ = 4
N_LAT = 4


def draw_topk_ids(key, part):
    rows_all = SEQS * LENGTH
    spacing = LATENTS // TOPK
    row_order = jax.random.permutation(jax.random.fold_in(key, 11), rows_all).astype(jnp.int32)
    shifts = jax.random.randint(jax.random.fold_in(key, 12), (TOPK,), 0, spacing).astype(jnp.int32)
    latent_order = jax.random.permutation(jax.random.fold_in(key, 13), LATENTS).astype(jnp.int32)
    offsets = (row_order[:, None] + shifts[None, :]) % spacing
    slots = jnp.arange(TOPK, dtype=jnp.int32)[None, :] * spacing + offsets
    chosen = latent_order[slots]
    return chosen.reshape(SEQS, LENGTH, TOPK).astype(jnp.int32)


def strengthened(array, stream_key, source, target, shards_of, factor):
    def block_of(axis_at):
        return (jnp.arange(array.shape[axis_at]) // (array.shape[axis_at] // shards_of)).reshape((-1,) + (1,) * (array.ndim - 1 - axis_at))

    one_side = jax.random.permutation(stream_key, shards_of)[block_of(target)]
    other_side = (block_of(target) + shards_of // 2) % shards_of
    return jnp.where((block_of(source) == one_side) | (block_of(source) == other_side), factor * array, array)


def shard_levels(rng, shape, shards, smallest, largest):
    level, own = 1.0, jax.random.fold_in(rng, 6)
    for axis_at, blocks in shards:
        draws = jnp.exp(jax.random.uniform(jax.random.fold_in(own, axis_at), (blocks,), jnp.float32, smallest / len(shards), largest / len(shards)))
        level = level * jnp.repeat(draws, shape[axis_at] // blocks).reshape([-1 if axis == axis_at else 1 for axis in range(len(shape))])
    return level


def scatter_about(own_key, extent, scale, limit, shards=(), kind=jnp.bfloat16):
    array = jax.random.normal(own_key, extent, jnp.float32) * scale
    if len(shards) > 0:
        array = shard_levels(own_key, extent, shards, -0.22, 0.18) * array
    return jnp.clip(array, min=-limit, max=limit).astype(kind)


def heavy_noise(rng, extent, spread, bound, cuts, heavy, kind=jnp.bfloat16):
    drawn = spread * jax.random.normal(rng, extent, jnp.float32)
    if cuts:
        drawn = drawn * shard_levels(rng, extent, cuts, -0.22, 0.18)
    return jnp.clip(strengthened(drawn, jax.random.fold_in(rng, 3), *heavy), -bound, bound).astype(kind)


def setup_inputs(seed: int = 0) -> dict:
    splits = jax.random.split(jax.random.key(seed), 6)
    activations = heavy_noise(splits[0], (SEQS, LENGTH, D), 1.0, 6.0, ((0, 2), (1, 4)), (1, 2, 4, 2.0))
    dictionary = scatter_about(splits[1], (LATENTS, D), D ** -0.5, 0.09375, ((0, 4),))
    topk_ids = draw_topk_ids(jax.random.fold_in(splits[5], 71), 0)
    kernel_taps = scatter_about(splits[3], (TAPS, LATENTS), TAPS ** -0.5, 2.0, ((1, 4),), jnp.float32)
    enc_bias = scatter_about(splits[4], (LATENTS,), 0.5, 3.0, ((0, 4),), jnp.float32)
    return dict(activations=activations, dictionary=dictionary, topk_ids=topk_ids, kernel_taps=kernel_taps, enc_bias=enc_bias)


def lagged(field, taps_block, forward):
    length = field.shape[1]
    padded = jnp.pad(field, ((0, 0), (HALF, HALF), (0, 0)))
    summed = jnp.zeros(field.shape, jnp.float32)
    for tap_index in range(TAPS):
        begin = tap_index if forward else 2 * HALF - tap_index
        summed = summed + taps_block[tap_index][None, None, :] * padded[:, begin:begin + length, :]
    return summed


def block_codes(token_wide, dict_block, taps_block, bias_block, topk_ids, first):
    latent_in = jnp.einsum("std,ld->stl", token_wide, dict_block.astype(jnp.float32))
    preact = lagged(latent_in, taps_block, True) + bias_block[None, None, :]
    width_block = dict_block.shape[0]
    inside = (topk_ids >= first) & (topk_ids < first + width_block)
    local_ids = jnp.where(inside, topk_ids - first, width_block).astype(jnp.int32)
    seq_ids = jnp.arange(topk_ids.shape[0], dtype=jnp.int32)[:, None, None]
    pos_ids = jnp.arange(topk_ids.shape[1], dtype=jnp.int32)[None, :, None]
    active = jnp.zeros(latent_in.shape, jnp.float32).at[seq_ids, pos_ids, local_ids].set(1.0, mode="drop")
    latents = (active * preact).astype(jnp.bfloat16)
    return latent_in, active, latents


def reference(activations, dictionary, topk_ids, kernel_taps, enc_bias):
    seqs, length, width = activations.shape
    tok_block = length // N_SEQ
    token_wide = activations.astype(jnp.float32)
    dict_blocks = dictionary.reshape(N_LAT, LAT_DEV, width)
    taps_blocks = kernel_taps.reshape(TAPS, N_LAT, LAT_DEV).transpose(1, 0, 2)
    bias_blocks = enc_bias.reshape(N_LAT, LAT_DEV)
    firsts = jnp.arange(N_LAT, dtype=jnp.int32) * LAT_DEV
    items = (dict_blocks, taps_blocks, bias_blocks, firsts)

    def decode(carry, item):
        dict_block, taps_block, bias_block, first = item
        unused_in, unused_active, latents = block_codes(token_wide, dict_block, taps_block, bias_block, topk_ids, first)
        part = jnp.einsum("stl,ld->std", latents.astype(jnp.float32), dict_block.astype(jnp.float32))
        return carry + part, None

    recon, unused = lax.scan(decode, jnp.zeros(activations.shape, jnp.float32), items)
    residual = (recon - token_wide).astype(jnp.bfloat16)
    resid_wide = residual.astype(jnp.float32)
    resid_blocks = resid_wide.reshape(seqs, N_SEQ, tok_block, width)
    token_blocks = token_wide.reshape(seqs, N_SEQ, tok_block, width)

    def backward(item):
        dict_block, taps_block, bias_block, first = item
        latent_in, active, latents = block_codes(token_wide, dict_block, taps_block, bias_block, topk_ids, first)
        grad_code = jnp.einsum("std,ld->stl", resid_wide, dict_block.astype(jnp.float32))
        grad_pre = active * grad_code
        grad_in = lagged(grad_pre, taps_block, False).astype(jnp.bfloat16)
        padded_in = jnp.pad(latent_in, ((0, 0), (HALF, HALF), (0, 0)))
        tap_grads = jnp.stack([jnp.sum(grad_pre * padded_in[:, tap_index:tap_index + length, :], axis=(0, 1)) for tap_index in range(TAPS)])
        bias_grads = jnp.sum(grad_pre, axis=(0, 1))
        code_blocks = latents.astype(jnp.float32).reshape(seqs, N_SEQ, tok_block, -1)
        grad_blocks = grad_in.astype(jnp.float32).reshape(seqs, N_SEQ, tok_block, -1)
        terms = jnp.einsum("sjtl,sjtd->sjld", code_blocks, resid_blocks) + jnp.einsum("sjtl,sjtd->sjld", grad_blocks, token_blocks)
        rounded = lax.optimization_barrier(terms.astype(jnp.bfloat16)).astype(jnp.float32)
        return jnp.sum(rounded, axis=(0, 1)), tap_grads, bias_grads

    dict_grads, tap_grads, bias_grads = lax.map(backward, items)
    grad_dictionary = dict_grads.reshape(N_LAT * LAT_DEV, width)
    grad_taps = tap_grads.transpose(1, 0, 2).reshape(TAPS, N_LAT * LAT_DEV)
    grad_bias = bias_grads.reshape(N_LAT * LAT_DEV)
    return grad_dictionary, grad_taps, grad_bias
```

```python
import functools

import jax
import jax.numpy as jnp
from jax import lax
from jax.experimental import pallas as pl
from jax.experimental.pallas import tpu as pltpu
from jax.sharding import PartitionSpec as P


LANES = 128
SUB = 8
TILE = 64
CHUNKS = (64, 64, 64, 64)
EARLY = 3
SPREADS = ((0, 1), (1, 1), (2, 2))


PICK_DIMS = lax.GatherDimensionNumbers(
    offset_dims=(),
    collapsed_slice_dims=(1,),
    start_index_map=(1,),
    operand_batching_dims=(0,),
    start_indices_batching_dims=(0,),
)


def lane_pick(rows, spots):
    return lax.gather(
        rows,
        spots[..., None],
        PICK_DIMS,
        (1, 1),
        mode=lax.GatherScatterMode.PROMISE_IN_BOUNDS,
    )


def by_latents(rows, block):
    return lax.dot_general(rows, block, (((1,), (1,)), ((), ())), preferred_element_type=jnp.float32)


def encode_kernel(rows_ref, dict_ref, out_ref, head_ref, tail_ref):
    cells = by_latents(rows_ref[...], dict_ref[...])
    out_ref[...] = cells
    head_ref[...] = cells[:SUB]
    tail_ref[...] = cells[cells.shape[0] - SUB :]


def encode(rows, dictionary):
    tokens, model = rows.shape
    width = dictionary.shape[0]
    step = 4 * LANES
    return pl.pallas_call(
        encode_kernel,
        grid=(width // step,),
        in_specs=[
            pl.BlockSpec((tokens, model), lambda i: (0, 0)),
            pl.BlockSpec((step, model), lambda i: (i, 0)),
        ],
        out_specs=[
            pl.BlockSpec((tokens, step), lambda i: (0, i)),
            pl.BlockSpec((SUB, step), lambda i: (0, i)),
            pl.BlockSpec((SUB, step), lambda i: (0, i)),
        ],
        out_shape=[
            jax.ShapeDtypeStruct((tokens, width), jnp.float32),
            jax.ShapeDtypeStruct((SUB, width), jnp.float32),
            jax.ShapeDtypeStruct((SUB, width), jnp.float32),
        ],
        name="encode",
    )(rows, dictionary)


def codes_kernel(
    spots_ref, taps_ref, bias_ref, map_ref, cells_ref, prev_ref, next_ref,
    codes_ref, line_ref, vals_ref, *, half
):
    tokens, lanes = cells_ref.shape
    tiles = lanes // LANES
    step = pl.program_id(0)
    for tile in range(tiles):
        across = slice(tile * LANES, (tile + 1) * LANES)
        line_ref[tile, 0:SUB, :] = prev_ref[:, across]
        line_ref[tile, SUB : SUB + tokens, :] = cells_ref[:, across]
        line_ref[tile, SUB + tokens :, :] = next_ref[:, across]

    @pl.when(step == 0)
    def _():
        vals_ref[...] = jnp.zeros(vals_ref.shape, jnp.float32)

    for part in range(tokens // TILE):
        at = slice(part * TILE, (part + 1) * TILE)
        spots = spots_ref[at, :]
        low = spots & (LANES - 1)
        high = spots >> 7
        picked = vals_ref[at, :]
        for tile in range(tiles):
            across = slice(tile * LANES, (tile + 1) * LANES)
            total = jnp.zeros((TILE, LANES), jnp.float32) + bias_ref[:, across]
            for k in range(2 * half + 1):
                start = SUB + part * TILE + k - half
                total = total + taps_ref[k : k + 1, across] * line_ref[tile, start : start + TILE, :]
            total = jnp.where(map_ref[at, across] > 0, total, 0.0)
            codes_ref[at, across] = total.astype(jnp.bfloat16)
            picked = jnp.where(high == step * tiles + tile, lane_pick(total, low), picked)
        vals_ref[at, :] = picked


def make_codes(spots, taps, bias, own_map, cells, before, behind):
    tokens, width = cells.shape
    step = 4 * LANES
    column = lambda rows: pl.BlockSpec((rows, step), lambda i: (0, i))
    whole = lambda a: pl.BlockSpec(a.shape, lambda i: (0, 0))
    return pl.pallas_call(
        functools.partial(codes_kernel, half=taps.shape[0] // 2),
        grid=(width // step,),
        in_specs=[
            whole(spots),
            column(taps.shape[0]),
            column(1),
            column(tokens),
            column(tokens),
            column(SUB),
            column(SUB),
        ],
        out_specs=[
            column(tokens),
            pl.BlockSpec((step // LANES, tokens + 2 * SUB, LANES), lambda i: (i, 0, 0)),
            pl.BlockSpec((tokens, LANES), lambda i: (0, 0)),
        ],
        out_shape=[
            jax.ShapeDtypeStruct((tokens, width), jnp.bfloat16),
            jax.ShapeDtypeStruct((width // LANES, tokens + 2 * SUB, LANES), jnp.float32),
            jax.ShapeDtypeStruct((tokens, LANES), jnp.float32),
        ],
        name="codes",
    )(spots, taps, bias, own_map, cells, before, behind)


def turned(stage_ref, rows_ref):
    for tile in range(rows_ref.shape[1] // LANES):
        at = slice(tile * LANES, (tile + 1) * LANES)
        stage_ref[at, :] = rows_ref[:, at].T


def dealt(order_ref, stage_ref, outs, wide):
    two = order_ref.shape[0] // len(outs) - 1
    for i, out_ref in enumerate(outs):
        for other in range(two):
            start = pl.multiple_of(order_ref[i * two + other] * wide, 2 * SUB)
            out_ref[other * wide : (other + 1) * wide, :] = stage_ref[pl.ds(start, wide), :]


def side_by_side(first, second):
    lanes = lax.broadcasted_iota(jnp.int32, first.shape, 1)
    moved = pltpu.roll(second.astype(jnp.float32), LANES // 2, 1)
    return jnp.where(lanes < LANES // 2, first.astype(jnp.float32), moved).astype(jnp.bfloat16)


def turned_half(stage_ref, rows_ref, start):
    for tile in range(rows_ref.shape[1] // LANES):
        at = slice(tile * LANES, (tile + 1) * LANES)
        cells = rows_ref[start : start + LANES // 2, at].astype(jnp.float32)
        both = jnp.concatenate([cells, cells], axis=0)
        stage_ref[at, :] = both.T.astype(jnp.bfloat16)


def dealt_half(order_ref, stage_ref, outs, wide, first):
    two = order_ref.shape[0] // len(outs) - 1
    for i, out_ref in enumerate(outs):
        cells = []
        for other in range(two):
            start = pl.multiple_of(order_ref[i * two + other] * wide, 2 * SUB)
            cells.append(stage_ref[pl.ds(start, wide), :])
        out_ref[first : first + wide, :] = side_by_side(*cells)


def share_kernel(order_ref, rows_ref, vals_ref, flat_ref, *refs, wide):
    outs, stage_ref = refs[:-1], refs[-1]
    turned(stage_ref, rows_ref)
    dealt(order_ref, stage_ref, outs, wide)
    tokens = rows_ref.shape[0]
    groups, line = flat_ref.shape
    first = (order_ref.shape[0] // len(outs) - 1) * wide
    cells = []
    for part in range(tokens // LANES):
        cells.append(vals_ref[part * LANES : (part + 1) * LANES, :])
    vals = jnp.concatenate(cells, axis=1).astype(jnp.bfloat16)
    flat = flat_ref[...]
    low = (flat & (LANES - 1)).astype(jnp.float32).astype(jnp.bfloat16)
    high = jnp.clip(flat >> 7, -1, LANES).astype(jnp.float32).astype(jnp.bfloat16)
    for out_ref in outs:
        out_ref[first : first + LANES, :] = vals
        start = first + LANES
        for ids in (low, high):
            for piece in range(line // tokens):
                out_ref[start : start + groups, :] = ids[:, piece * tokens : (piece + 1) * tokens]
                start += groups


def shared_columns(order, rows, vals, flat, count):
    total, model = rows.shape
    blocks = order.shape[0] - count
    wide = model // blocks
    height = blocks // count * wide + LANES + 2 * flat.shape[0] * flat.shape[1] // total
    vmem = pl.BlockSpec(memory_space=pltpu.VMEM)
    return pl.pallas_call(
        functools.partial(share_kernel, wide=wide),
        in_specs=[pl.BlockSpec(memory_space=pltpu.SMEM), vmem, vmem, vmem],
        out_shape=[jax.ShapeDtypeStruct((height, total), jnp.bfloat16)] * count,
        scratch_shapes=[pltpu.VMEM((model, total), jnp.bfloat16)],
        name="shared_columns",
    )(order, rows, vals, flat)


def error_kernel(order_ref, outer_ref, rows_ref, *refs, pieces, wide):
    got = refs[: 2 * pieces]
    err_ref, outs, (stage_ref, half_ref) = refs[2 * pieces], refs[2 * pieces + 1 : -2], refs[-2:]
    outer = outer_ref[0] > 0
    start = 0
    for piece in range(pieces):
        near_ref, far_ref = got[2 * piece], got[2 * piece + 1]
        count = near_ref.shape[0]
        total = jnp.where(outer, far_ref[...], near_ref[...]).astype(jnp.float32)
        error = total - rows_ref[start : start + count, :].astype(jnp.float32)
        err_ref[start : start + count, :] = error.astype(jnp.bfloat16)
        start += count
    for tile in range(err_ref.shape[1] // LANES):
        at = slice(tile * LANES, (tile + 1) * LANES)
        stage_ref[at, :] = err_ref[:LANES, at].T
    dealt(order_ref, stage_ref, outs, wide)
    turned_half(half_ref, err_ref, LANES)
    dealt_half(order_ref, half_ref, outs, wide, (order_ref.shape[0] // len(outs) - 1) * wide)


def error_columns(order, outer, rows, nears, fars, count):
    model = rows.shape[1]
    total = sum(near.shape[0] for near in nears)
    blocks = order.shape[0] - count
    wide = model // blocks
    pairs = [array for pair in zip(nears, fars) for array in pair]
    smem = pl.BlockSpec(memory_space=pltpu.SMEM)
    vmem = pl.BlockSpec(memory_space=pltpu.VMEM)
    return pl.pallas_call(
        functools.partial(error_kernel, pieces=len(nears), wide=wide),
        in_specs=[smem, smem, vmem] + [vmem] * len(pairs),
        out_shape=[jax.ShapeDtypeStruct((total, model), jnp.bfloat16)]
        + [jax.ShapeDtypeStruct(((blocks // count + 1) * wide, LANES), jnp.bfloat16)] * count,
        scratch_shapes=[pltpu.VMEM((model, LANES), jnp.bfloat16)] * 2,
        name="error_columns",
    )(order, outer, rows, *pairs)


def grad_kernel(
    order_ref, outer_ref, spots_ref, rows_ref, early_ref, near_ref, far_ref, dict_ref, map_ref,
    padded_ref, *refs, taps_count, steps
):
    outs, (err_ref, stage_ref, picked_ref) = refs[:-3], refs[-3:]
    tokens, model = rows_ref.shape
    cut = early_ref.shape[0]
    step = pl.program_id(0)
    lanes = dict_ref.shape[0] // LANES
    small = tokens
    half = taps_count // 2

    @pl.when(step == 0)
    def _():
        err_ref[0:cut, :] = early_ref[...]
        total = jnp.where(outer_ref[0] > 0, far_ref[...], near_ref[...]).astype(jnp.float32)
        error = total - rows_ref[cut:, :].astype(jnp.float32)
        err_ref[cut:, :] = error.astype(jnp.bfloat16)
        picked_ref[...] = jnp.zeros(picked_ref.shape, jnp.float32)

    code = by_latents(err_ref[...], dict_ref[...])

    @pl.when(step == 0)
    def _():
        turned_half(stage_ref, err_ref, cut)
        wide = model // (order_ref.shape[0] - len(outs))
        dealt_half(order_ref, stage_ref, outs, wide, small + 2 * SUB * lanes * steps)

    for block in range(lanes):
        part = code[:, block * LANES : (block + 1) * LANES]
        sums = []
        live = jnp.where(map_ref[:, block * LANES : (block + 1) * LANES] > 0, part, 0.0)
        for k in range(taps_count):
            start = SUB + k - half
            seen = padded_ref[block, start : start + tokens, :]
            sums.append(jnp.sum(live * seen, axis=0, keepdims=True))
        sums.append(jnp.sum(live, axis=0, keepdims=True))
        sums.append(jnp.zeros((2 * SUB - len(sums), LANES), jnp.float32))
        rows16 = jnp.concatenate(sums, axis=0).astype(jnp.bfloat16)
        spot = pl.multiple_of(small + (step * lanes + block) * 2 * SUB, 2 * SUB)
        for out_ref in outs:
            out_ref[pl.ds(spot, 2 * SUB), :] = rows16
        for piece in range(tokens // TILE):
            at = slice(piece * TILE, (piece + 1) * TILE)
            spots = spots_ref[at, :]
            got = lane_pick(part[at, :], spots & (LANES - 1))
            picked_ref[at, :] = picked_ref[at, :] + jnp.where(
                spots >> 7 == step * lanes + block, got, 0.0
            )

    @pl.when(step == pl.num_programs(0) - 1)
    def _():
        vals = picked_ref[...].astype(jnp.bfloat16)
        for out_ref in outs:
            out_ref[0:tokens, :] = vals


def grad_messages(order, outer, spots, rows, early, near, far, dictionary, own_map, padded, taps_count, count):
    tokens, model = rows.shape
    width = dictionary.shape[0]
    step = 4 * LANES
    blocks = order.shape[0] - count
    wide = model // blocks
    first = tokens + 2 * SUB * width // LANES
    total = first + wide
    smem = pl.BlockSpec(memory_space=pltpu.SMEM)
    whole = lambda a: pl.BlockSpec(a.shape, lambda i: (0, 0))
    column = lambda rows: pl.BlockSpec((rows, step), lambda i: (0, i))
    outs = pl.pallas_call(
        functools.partial(grad_kernel, taps_count=taps_count, steps=width // step),
        grid=(width // step,),
        in_specs=[
            smem,
            smem,
            whole(spots),
            whole(rows),
            whole(early),
            whole(near),
            whole(far),
            pl.BlockSpec((step, model), lambda i: (i, 0)),
            column(tokens),
            pl.BlockSpec((step // LANES, tokens + 2 * SUB, LANES), lambda i: (i, 0, 0)),
        ],
        out_specs=[pl.BlockSpec((total, LANES), lambda i: (0, 0))] * count,
        out_shape=[jax.ShapeDtypeStruct((total, LANES), jnp.bfloat16)] * count,
        scratch_shapes=[
            pltpu.VMEM((tokens, model), jnp.bfloat16),
            pltpu.VMEM((model, LANES), jnp.bfloat16),
            pltpu.VMEM((tokens, LANES), jnp.float32),
        ],
        name="grad_messages",
    )(order, outer, spots, rows, early, near, far, dictionary, own_map, padded)
    return outs, first


def slot_tile(low, high, slots, blocks):
    wide = low.shape[1]
    lane = lax.broadcasted_iota(jnp.int32, (1, wide), 1)
    token = lane // slots
    slot = (lane - token * slots + 1).astype(jnp.float32)
    inside = (high >= 0) & (high < blocks)
    code = jnp.where(inside, high * SUB + token, -1)
    rows = lax.broadcasted_iota(jnp.int32, (blocks * SUB, wide), 0)
    left = jnp.where(rows == code, slot, 0.0).astype(jnp.bfloat16)
    cols = lax.broadcasted_iota(jnp.int32, (LANES, wide), 0)
    right = jnp.where(cols == low, 1.0, 0.0).astype(jnp.bfloat16)
    return lax.dot_general(
        left, right, (((1,), (1,)), ((), ())), preferred_element_type=jnp.float32
    )


def map_kernel(flat_ref, map_ref, *, slots):
    blocks = map_ref.shape[1] // LANES
    for group in range(flat_ref.shape[0]):
        flat = flat_ref[group : group + 1, :]
        tile = slot_tile(flat & (LANES - 1), flat >> 7, slots, blocks)
        for block in range(blocks):
            map_ref[group * SUB : (group + 1) * SUB, block * LANES : (block + 1) * LANES] = tile[
                block * SUB : (block + 1) * SUB
            ].astype(jnp.int32)


def slot_map(flat, slots, width):
    groups = flat.shape[0]
    step = 16
    return pl.pallas_call(
        functools.partial(map_kernel, slots=slots),
        grid=(groups // step,),
        in_specs=[pl.BlockSpec((step, flat.shape[1]), lambda i: (i, 0))],
        out_specs=pl.BlockSpec((step * SUB, width), lambda i: (i, 0)),
        out_shape=jax.ShapeDtypeStruct((groups * SUB, width), jnp.int32),
        name="slot_map",
    )(flat)


def spread_kernel(*refs, slots, count):
    vals_refs, ids_refs = refs[:count], refs[count : 2 * count]
    map_ref, dense_ref, wide_ref = refs[-3:]
    blocks = map_ref.shape[2] // LANES
    ids_rows, line = ids_refs[0].shape
    pieces = SUB * slots // line
    groups = ids_rows // 2 // pieces
    step = map_ref.shape[1] // SUB
    first = pl.program_id(0) * step

    @pl.when(pl.program_id(0) == 0)
    def _():
        for r, ids_ref in enumerate(ids_refs):
            wide_ref[r] = ids_ref[...].astype(jnp.float32)

    for pair in range(step // 2):
        at = slice(pair * 2 * SUB, (pair + 1) * 2 * SUB)
        for r in range(count):
            both = vals_refs[r][at, :].astype(jnp.float32)
            outs = []
            for half in range(2):
                group = first + pair * 2 + half
                parts = []
                for which in range(2):
                    cells = [
                        wide_ref[r, pl.ds((which * pieces + piece) * groups + group, 1), :]
                        for piece in range(pieces)
                    ]
                    parts.append(jnp.concatenate(cells, axis=1).astype(jnp.int32))
                tile = slot_tile(parts[0], parts[1], slots, blocks)
                vals = both[half * SUB : (half + 1) * SUB]
                row = []
                for block in range(blocks):
                    found = tile[block * SUB : (block + 1) * SUB].astype(jnp.int32)
                    spot = jnp.where(found > 0, found - 1, slots)
                    row.append((spot, lane_pick(vals, spot)))
                outs.append(row)
            for block in range(blocks):
                lanes = slice(block * LANES, (block + 1) * LANES)
                spots = jnp.concatenate([outs[0][block][0], outs[1][block][0]], axis=0)
                cells = jnp.concatenate([outs[0][block][1], outs[1][block][1]], axis=0)
                map_ref[r, at, lanes] = spots
                dense_ref[r, at, lanes] = cells.astype(jnp.bfloat16)


def spread(heard, at, total, first, slots, tokens, width, made):
    count = len(heard)
    line = heard[0].shape[1]
    ids = heard[0].shape[0] - first - LANES
    vals_at, ids_at = first // LANES, (first + LANES) // ids
    dense_at = total // count + at
    return pl.pallas_call(
        functools.partial(spread_kernel, slots=slots, count=count),
        grid=(tokens // LANES,),
        in_specs=[pl.BlockSpec((LANES, LANES), lambda i: (vals_at, i))] * count
        + [pl.BlockSpec((ids, line), lambda i: (ids_at, 0))] * count
        + [pl.BlockSpec(memory_space=pl.ANY)] * len(made),
        out_specs=[
            pl.BlockSpec((count, LANES, width), lambda i: (at, i, 0)),
            pl.BlockSpec((count, LANES, width), lambda i: (dense_at, i, 0)),
        ],
        out_shape=[
            jax.ShapeDtypeStruct((total, tokens, width), jnp.int32),
            jax.ShapeDtypeStruct((2 * total, tokens, width), jnp.bfloat16),
        ],
        input_output_aliases={2 * count + i: i for i in range(len(made))},
        scratch_shapes=[pltpu.VMEM((count, ids, line), jnp.float32)],
        name="spread",
    )(*heard, *heard, *made)


def lag_kernel(where_ref, taps_ref, map_ref, pair_ref, *refs, half):
    count, tokens, lanes = map_ref.shape
    base = where_ref.shape[0] - count
    vals_refs, out_ref, line_ref = refs[:count], refs[count], refs[count + 1]
    for tile in range(lanes // LANES):
        across = slice(tile * LANES, (tile + 1) * LANES)
        for block in range(count):
            for part in range(tokens // TILE):
                at = slice(part * TILE, (part + 1) * TILE)
                vals = vals_refs[block][at, :].astype(jnp.float32)
                start = SUB + part * TILE
                line_ref[tile, block, start : start + TILE, :] = lane_pick(
                    vals, map_ref[block, at, across]
                )
        for block in range(count):
            place = where_ref[base + block]
            before, behind = jnp.int32(0), jnp.int32(0)
            for other in range(count):
                before = jnp.where(where_ref[base + other] == place - 1, other, before)
                behind = jnp.where(where_ref[base + other] == place + 1, other, behind)
            last = line_ref[tile, before, tokens : tokens + SUB, :]
            line_ref[tile, block, 0:SUB, :] = jnp.where(place > 0, last, 0.0)
            head = line_ref[tile, behind, SUB : 2 * SUB, :]
            line_ref[tile, block, tokens + SUB :, :] = jnp.where(place < count - 1, head, 0.0)
        taps = [taps_ref[k : k + 1, across] for k in range(2 * half + 1)]
        for block in range(count):
            for part in range(tokens // TILE):
                total = jnp.zeros((TILE, LANES), jnp.float32)
                for k in range(2 * half + 1):
                    start = SUB + part * TILE + half - k
                    total = total + taps[k] * line_ref[tile, block, start : start + TILE, :]
                out_ref[block, part * TILE : (part + 1) * TILE, across] = total.astype(jnp.bfloat16)


def add_lagged(where, taps, slots_at, messages, pair):
    count, tokens, width = slots_at.shape
    step = 2 * LANES
    column = pl.BlockSpec((count, tokens, step), lambda i: (0, 0, i))
    return pl.pallas_call(
        functools.partial(lag_kernel, half=taps.shape[0] // 2),
        grid=(width // step,),
        in_specs=[
            pl.BlockSpec(memory_space=pltpu.SMEM),
            pl.BlockSpec((taps.shape[0], step), lambda i: (0, i)),
            column,
            pl.BlockSpec(memory_space=pl.ANY),
        ]
        + [pl.BlockSpec((tokens, LANES), lambda i: (0, 0))] * count,
        out_specs=column,
        out_shape=jax.ShapeDtypeStruct(pair.shape, pair.dtype),
        input_output_aliases={3: 0},
        scratch_shapes=[pltpu.VMEM((step // LANES, count, tokens + 2 * SUB, LANES), jnp.float32)],
        name="add_lagged",
    )(where, taps, slots_at, pair, *messages)


def left_kernel(*refs, count, first, tokens):
    own, early, rest = refs[:count], refs[count : 2 * count], refs[2 * count : 3 * count]
    message = refs[3 * count : 4 * count]
    out_ref, small_ref, stage_ref = refs[4 * count :]
    wide = own[0].shape[0]
    which = pl.program_id(0)
    lanes = lax.broadcasted_iota(jnp.int32, (wide, LANES), 1)
    left = lanes < LANES // 2
    for r in range(count):
        out_ref[0, :, r * tokens : (r + 1) * tokens] = own[r][...]
        base = (count + r) * tokens
        out_ref[0, :, base : base + LANES] = early[r][...]
        middle = rest[r][...].astype(jnp.float32)
        late = message[r][first:, :].astype(jnp.float32)
        kept = jnp.where(left, middle, pltpu.roll(late, LANES // 2, 1))
        passed = jnp.where(left, pltpu.roll(middle, LANES // 2, 1), late)
        both = jnp.where(which == 0, kept, passed)
        out_ref[0, :, base + LANES : base + tokens] = both.astype(jnp.bfloat16)

    @pl.when(which == 0)
    def _():
        total = jnp.zeros(stage_ref.shape, jnp.float32)
        for r in range(count):
            total = total + message[r][tokens:first, :].astype(jnp.float32)
        stage_ref[...] = total
        for block in range(stage_ref.shape[0] // (2 * SUB)):
            small_ref[:, block * LANES : (block + 1) * LANES] = stage_ref[
                block * 2 * SUB : (block + 1) * 2 * SUB, :
            ]


def left_operands(own, early, messages, first, wide, width):
    count = len(own)
    tokens = own[0].shape[1]
    piece = lambda a: pl.BlockSpec((wide, a.shape[1]), lambda i: (i, 0))
    whole = lambda a: pl.BlockSpec(a.shape, lambda i: (0, 0))
    return pl.pallas_call(
        functools.partial(left_kernel, count=count, first=first, tokens=tokens),
        grid=(2,),
        in_specs=[piece(a) for a in (*own, *early)]
        + [pl.BlockSpec((wide, LANES), lambda i: (2, 0))] * count
        + [whole(a) for a in messages],
        out_specs=[
            pl.BlockSpec((1, wide, 2 * count * tokens), lambda i: (i, 0, 0)),
            pl.BlockSpec((2 * SUB, width), lambda i: (0, 0)),
        ],
        out_shape=[
            jax.ShapeDtypeStruct((2, wide, 2 * count * tokens), jnp.bfloat16),
            jax.ShapeDtypeStruct((2 * SUB, width), jnp.float32),
        ],
        scratch_shapes=[pltpu.VMEM((first - tokens, LANES), jnp.float32)],
        name="left_operands",
    )(*own, *early, *early, *messages)


def after(value, *earlier):
    return lax.optimization_barrier((value, *earlier))[0]


class Plane:
    def __init__(self):
        self.seqs = lax.axis_size("batch")
        self.his = lax.axis_size("seq") // self.seqs
        place = lax.axis_index("seq")
        self.hi = place // self.seqs
        self.lo = place % self.seqs
        self.seq = lax.axis_index("batch")

    def shifts(self):
        return [(a, b) for b in range(self.seqs) for a in range(self.his)]

    def perm(self, a, b):
        pairs = []
        for hi in range(self.his):
            for lo in range(self.seqs):
                for seq in range(self.seqs):
                    source = (hi * self.seqs + lo) * self.seqs + seq
                    to_hi = (hi + a) % self.his
                    to_seq = (lo + b) % self.seqs
                    pairs.append((source, (to_hi * self.seqs + seq) * self.seqs + to_seq))
        return pairs

    def send(self, block, a, b):
        return lax.ppermute(block, ("seq", "batch"), self.perm(a, b))

    def send_all(self, blocks):
        return [self.send(block, a, b) for block, (a, b) in zip(blocks, self.shifts())]

    def true_blocks(self):
        return [
            ((self.hi - a) % self.his) * self.seqs + (self.seq - b) % self.seqs
            for a, b in self.shifts()
        ]

    def column_order(self):
        order = []
        for a, b in self.shifts():
            to_hi = (self.hi + a) % self.his
            to_seq = (self.lo + b) % self.seqs
            for other in range(self.seqs):
                lo = (self.seq + other) % self.seqs
                order.append((to_hi * self.seqs + lo) * self.seqs + to_seq)
        return jnp.stack(order + self.true_blocks()).astype(jnp.int32)


def permute(block, axis, pairs):
    return lax.ppermute(block, axis, pairs)


def steps(activations, dictionary, topk_ids, kernel_taps, enc_bias):
    plane = Plane()
    rows = activations[0]
    tokens, model = rows.shape
    width = dictionary.shape[0]
    taps_count = kernel_taps.shape[0]
    slots = topk_ids.shape[2]
    names = ["q%d" % i for i in range(len(plane.shifts()))]
    shifts = len(names)
    order = plane.column_order()
    columns_in_all = shifts * plane.seqs
    line = lax.axis_size("lat")
    place = lax.axis_index("lat")
    outer = ((place == 0) | (place == line - 1)).astype(jnp.int32).reshape(1)
    local = topk_ids[0] - place * width
    flat = local.reshape(tokens // SUB, SUB * slots)
    spots = jnp.pad(local, ((0, 0), (0, LANES - slots)), constant_values=-1)

    cells, head, tail = encode(rows, dictionary)
    ends = range(lax.axis_size("seq") - 1)
    before = permute(tail, "seq", [(i, i + 1) for i in ends])
    behind = permute(head, "seq", [(i + 1, i) for i in ends])
    own_map = slot_map(flat, slots, width)
    codes, padded, vals = make_codes(
        spots, kernel_taps, enc_bias[None, :], own_map, cells, before, behind
    )
    count = len(CHUNKS)
    starts = [sum(CHUNKS[:i]) for i in range(count + 1)]
    recon = jnp.dot(codes, dictionary, preferred_element_type=jnp.float32).astype(jnp.bfloat16)
    parts = [after(recon[starts[i] : starts[i + 1]]) for i in range(count)]
    near, across, totals, finals = {}, {}, {}, {}
    if line == 4:
        inward = [permute(part, "lat", [(0, 1), (3, 2)]) for part in parts]
        for i in range(count):
            got = after(inward[i], near[i - 1]) if i else inward[i]
            near[i] = jnp.add(parts[i], got)
            across[i] = permute(near[i], "lat", [(1, 2), (2, 1)])
        for i in range(count):
            got = after(across[i], totals[i - 1]) if i else across[i]
            totals[i] = jnp.add(near[i], got)
            finals[i] = permute(totals[i], "lat", [(1, 0), (2, 3)])
    else:
        for i, part in enumerate(parts):
            totals[i] = finals[i] = lax.psum(part, "lat")

    def send(i, block):
        a, b = plane.shifts()[i]
        return permute(block, ("seq", "batch"), plane.perm(a, b))

    columns = shared_columns(order, rows, vals, flat, shifts)
    own = [send(i, columns[i]) for i in range(shifts)]

    early = error_columns(
        order,
        outer,
        rows,
        [totals[i] for i in range(EARLY)],
        [finals[i] for i in range(EARLY)],
        shifts,
    )
    early_errors = [send(i, early[1 + i]) for i in range(shifts)]
    late_near = jnp.concatenate([totals[i] for i in range(EARLY, count)], axis=0)
    late_far = jnp.concatenate([finals[i] for i in range(EARLY, count)], axis=0)
    messages, first = grad_messages(
        order,
        outer,
        spots,
        rows,
        early[0],
        late_near,
        late_far,
        dictionary,
        own_map,
        padded,
        taps_count,
        shifts,
    )
    messages = [send(i, messages[i]) for i in range(shifts)]
    wide = model // columns_in_all
    made = ()
    for start, size in SPREADS:
        part = own[start : start + size]
        made = spread(part, start // size, shifts, wide * plane.seqs, slots, tokens, width, made)
    slots_at, pair = made
    lefts, small = left_operands(own, early_errors, messages, first, wide, width)
    pair = add_lagged(order, kernel_taps, slots_at, messages, pair)
    right = pair.reshape(-1, width)
    seqs = plane.seqs
    swap = [(s, s - s % seqs + (s + 1) % seqs) for s in range(lax.axis_size("seq"))]
    sent = jnp.dot(lefts[1], right, preferred_element_type=jnp.float32).astype(jnp.bfloat16)
    other = permute(sent, "seq", swap)
    small = small + permute(small, "seq", swap)
    total = jnp.dot(lefts[0], right, preferred_element_type=jnp.float32)
    total = total + other.astype(jnp.float32)
    return total.T, small[:taps_count], small[taps_count]


def solution(mesh):
    return jax.shard_map(
        steps,
        mesh=mesh,
        in_specs=(
            P("batch", "seq", None),
            P("lat", None),
            P("batch", "seq", None),
            P(None, "lat"),
            P("lat"),
        ),
        out_specs=(P("lat", ("seq", "batch")), P(None, "lat"), P("lat")),
        check_vma=False,
    )
```
